32 devices in a mesh: dp: 2 (over x), expert: 16 (over z, y, core).
Axes of the slice: x: 2, y: 2, z: 4, core: 2. Of those that a mesh axis runs over, the one named last changes fastest.
Arguments:
- tokens: bfloat16 [4096, 2048], P(('dp', 'expert')), may hold values from -6 to 6
- grad_out: bfloat16 [4096, 2048], P(('dp', 'expert')), may hold values from -0.125 to 0.125
- router_weight: bfloat16 [2048, 16], replicated, may hold values from -0.125 to 0.125
- expert_index: int32 [4096, 8], P(('dp', 'expert')), may hold values from 0 to 15, all different within a row; in each aligned block of 128 rows (0 to 127, 128 to 255, ...) at most 96 rows name the same one
- w_gate: bfloat16 [16, 2048, 768], P('expert'), may hold values from -0.125 to 0.125
- w_up: bfloat16 [16, 2048, 768], P('expert'), may hold values from -0.125 to 0.125
- w_down: bfloat16 [16, 768, 2048], P('expert'), may hold values from -0.21875 to 0.21875
Outputs:
- gate_grad: float32 [4096, 8], P(('dp', 'expert'))
- router_grad: float32 [2048, 16], P('expert')
The draws below stay inside these ranges and needn't reach their ends.
Inputs may be any that keep to these rules, and one draw needn't show every extreme that they name: `expert_index`: each row names 8 different experts. In each aligned block of 128 rows (the rows of one device) no expert is named by more than 96 rows, a bound that some blocks reach.
All inputs are finite; a program needn't handle non-finite values.
Results may differ from the reference program's by a relative error of at most 0.009.
Values may be sent and summed in bfloat16 or wider, within the bound.
A program may use at most 128 MiB of HBM per device.

```python
import math
import jax
import jax.numpy as jnp
import numpy as np
from jax import lax

D = 2048
FF = 768
TOP = 8
TOK_DEV = 128
EXPERTS = 16
CAP = 96
TOKENS = 4096


def spiked(array, stream_key, source, target, shards_of, factor):
    def block_of(position):
        return (jnp.arange(array.shape[position]) // (array.shape[position] // shards_of)).reshape((-1,) + (1,) * (array.ndim - 1 - position))

    one_side = jax.random.permutation(stream_key, shards_of)[block_of(target)]
    second = (block_of(target) + shards_of // 2) % shards_of
    return jnp.where((block_of(source) == one_side) | (block_of(source) == second), factor * array, array)


def steps_of(stream_key, dims, shards, least, high):
    loudness = 1.0
    for dim, parts in shards:
        heights = jax.random.uniform(jax.random.fold_in(jax.random.fold_in(stream_key, 6), dim), (parts,), jnp.float32, least / len(shards), high / len(shards))
        loudness = loudness * jnp.repeat(jnp.exp(heights), dims[dim] // parts).reshape((-1,) + (1,) * (len(dims) - 1 - dim))
    return loudness


def deal_out(rng, own, number, rows, count, top, most, slope):
    ranking = jax.random.permutation(rng, count)
    heavy_load, common = portions_of(count, rows * top, most, slope, True), portions_of(count, rows * top, most, slope, False)
    places = jnp.arange(count)

    def named(sizes, rotation):
        used = int((sizes > 0).sum())
        fixed = max(1, used // 4)
        shifted = fixed + (places - fixed + rotation * (used - fixed)) % max(1, count - fixed)
        return jnp.zeros((count,), jnp.int32).at[ranking[jnp.where(places < fixed, places, shifted)]].set(jnp.asarray(sizes, jnp.int32))

    sizes = jnp.where(number % 4 == 0, named(heavy_load, number // 4), named(common, number - number // 4 - 1))
    mixed = jax.random.permutation(jax.random.fold_in(own, 3), count)
    donor, taker = mixed[0:count // 2 * 2:2], mixed[1:count // 2 * 2:2]
    margin = jnp.minimum(sizes[donor] - 1, most - sizes[taker]) // 2
    margin = jnp.where((donor == ranking[0]) | (taker == ranking[0]) | (sizes[taker] == 0), 0, jnp.maximum(margin, 0))
    shifted = jax.random.randint(jax.random.fold_in(own, 4), (count // 2,), 0, 1 << 20) % (margin + 1)
    sizes = sizes.at[donor].add(-shifted).at[taker].add(shifted)
    items = jnp.searchsorted(jnp.cumsum(sizes), jnp.arange(rows * top), side="right").astype(jnp.int32)
    listing = items.reshape(top, rows).T
    listing = listing[jax.random.permutation(jax.random.fold_in(own, 1), rows)]
    rotation = jax.random.randint(jax.random.fold_in(own, 2), (rows, 1), 0, top)
    return jnp.take_along_axis(listing, (jnp.arange(top)[None, :] + rotation) % top, axis=1)


def portions_of(number_of, total, bound, slope, full):
    weights = [(1 << 20) // math.isqrt(standing ** slope) + 1 for standing in range(1, number_of + 1)]
    largest = bound if full else min(bound, max(-(-total // number_of), total * weights[0] // sum(weights)))
    least = 1 if total - largest >= number_of - 1 else 0
    counts, rest = [largest] + [least] * (number_of - 1), total - largest - least * (number_of - 1)
    while rest > 0:
        movable = [i for i in range(1, number_of) if counts[i] < largest] or [i for i in range(1, number_of) if counts[i] < bound]
        whole, remaining = sum([weights[i] for i in movable]), rest
        for i in movable:
            extra = min(bound - counts[i], max(1, remaining * weights[i] // whole), rest)
            counts[i] = counts[i] + extra
            rest = rest - extra
    return np.array(counts)


def bell_draw(stream_key, dims, width, most, pieces=(), held_as=jnp.bfloat16):
    gain = steps_of(stream_key, dims, pieces, -0.22, 0.18) if pieces else 1.0
    result = jax.random.normal(stream_key, dims, jnp.float32) * width * gain
    return jnp.minimum(jnp.maximum(result, -most), most).astype(held_as)


def gaussian_with(key, extent, spread, bound, shards, heavy, held_as=jnp.bfloat16):
    values = spread * jax.random.normal(key, extent, jnp.float32)
    if shards:
        values = values * steps_of(key, extent, shards, -0.22, 0.18)
    return jnp.clip(spiked(values, jax.random.fold_in(key, 3), *heavy), -bound, bound).astype(held_as)


def setup_inputs(seed: int = 0) -> dict:
    keys = jax.random.split(jax.random.key(seed), 8)
    tokens = gaussian_with(keys[0], (TOKENS, D), 1.0, 6.0, ((0, 32),), (0, 1, 32, 2.75))
    grad_out = bell_draw(keys[1], (TOKENS, D), D ** -0.5, 0.125, ((0, 32),))
    router_weight = bell_draw(keys[2], (D, EXPERTS), D ** -0.5, 0.125)
    expert_index_keys = jax.random.split(jax.random.fold_in(keys[3], 1), TOKENS // TOK_DEV)
    expert_index_turns = jax.random.permutation(jax.random.fold_in(keys[3], 3), TOKENS // TOK_DEV)
    expert_index = jax.vmap(lambda own, number: deal_out(jax.random.fold_in(keys[3], 2), own, number, TOK_DEV, EXPERTS, TOP, CAP, 2))(expert_index_keys, expert_index_turns).reshape((TOKENS, TOP))
    w_gate = bell_draw(keys[4], (EXPERTS, D, FF), D ** -0.5, 0.125, ((0, 16),))
    w_up = bell_draw(keys[5], (EXPERTS, D, FF), D ** -0.5, 0.125, ((0, 16),))
    w_down = bell_draw(keys[6], (EXPERTS, FF, D), FF ** -0.5, 0.21875, ((0, 16),))
    return dict(tokens=tokens, grad_out=grad_out, router_weight=router_weight, expert_index=expert_index, w_gate=w_gate, w_up=w_up, w_down=w_down)


def slot_table(expert_index):
    blocks = expert_index.reshape(-1, TOK_DEV, TOP)
    labels = jnp.arange(EXPERTS, dtype=jnp.int32)
    hits = (blocks[..., None] == labels).astype(jnp.int32)
    per_token = jnp.sum(hits, axis=2)
    before = jnp.cumsum(per_token, axis=1) - per_token
    slot = jnp.sum(hits * before[:, :, None, :], axis=3)
    return slot.reshape(-1, TOP).astype(jnp.int32)


def reference(tokens, grad_out, router_weight, expert_index, w_gate, w_up, w_down):
    slot = slot_table(expert_index)
    blocks = TOKENS // TOK_DEV
    token_ids = jnp.broadcast_to(jnp.arange(TOKENS, dtype=jnp.int32)[:, None], (TOKENS, TOP))
    source = (token_ids // TOK_DEV).astype(jnp.int32)
    column = (source * CAP + slot).astype(jnp.int32)
    table = jnp.zeros((EXPERTS, blocks * CAP), jnp.int32).at[expert_index, column].set(token_ids)

    def one_expert(which):
        picked = table[which]
        rows = tokens[picked]
        gate_in = jnp.dot(rows, w_gate[which], preferred_element_type=jnp.float32)
        up_in = jnp.dot(rows, w_up[which], preferred_element_type=jnp.float32)
        hidden = (jax.nn.silu(gate_in) * up_in).astype(jnp.bfloat16)
        expert_out = jnp.dot(hidden, w_down[which], preferred_element_type=jnp.float32).astype(jnp.bfloat16)
        return jnp.sum(expert_out.astype(jnp.float32) * grad_out[picked].astype(jnp.float32), axis=1)

    dots = lax.map(one_expert, jnp.arange(EXPERTS, dtype=jnp.int32))
    gate_grad = dots[expert_index, column]

    logits = jnp.dot(tokens, router_weight, preferred_element_type=jnp.float32)
    chosen = jnp.take_along_axis(logits, expert_index, axis=1)
    weights = jnp.exp(chosen)
    gates = weights / jnp.sum(weights, axis=1, keepdims=True)
    mean_term = jnp.sum(gates * gate_grad, axis=1, keepdims=True)
    logit_grad = gates * (gate_grad - mean_term)
    labels = jnp.arange(EXPERTS, dtype=jnp.int32)
    hits = (expert_index[:, :, None] == labels).astype(jnp.float32)
    dense = jnp.sum(logit_grad[:, :, None] * hits, axis=1)
    router_grad = jnp.dot(tokens.astype(jnp.float32).T, dense, precision=lax.Precision.HIGHEST)
    return gate_grad, router_grad
```

```python
import jax
import jax.numpy as jnp
from jax import lax
from jax.sharding import PartitionSpec as P


def on_device(tokens, grad_out, router_weight, expert_index, w_gate, w_up, w_down):
    tok_rows, width = tokens.shape
    top = expert_index.shape[1]
    experts = router_weight.shape[1]
    me = lax.axis_index("expert")
    n = lax.axis_size("expert")
    index_all = lax.all_gather(expert_index, "expert", axis=0, tiled=True)
    tok_all = lax.all_gather(tokens, "expert", axis=0, tiled=True)
    grad_all = lax.all_gather(grad_out, "expert", axis=0, tiled=True)
    gate_in = jnp.dot(tok_all, w_gate[0], preferred_element_type=jnp.float32)
    up_in = jnp.dot(tok_all, w_up[0], preferred_element_type=jnp.float32)
    hidden = jax.nn.silu(gate_in) * up_in
    back = lax.dot_general(
        grad_all, w_down[0], (((1,), (1,)), ((), ())), preferred_element_type=jnp.float32
    )
    dots = jnp.sum(hidden * back, axis=1)
    dots_all = lax.all_gather(dots, "expert", axis=0).T
    labels = jnp.arange(experts, dtype=jnp.int32)
    picked = jnp.any(index_all[:, :, None] == labels, axis=1)
    logits = jnp.dot(tok_all, router_weight, preferred_element_type=jnp.float32)
    weights = jnp.where(picked, jnp.exp(jnp.where(picked, logits, 0.0)), 0.0)
    gates = weights / jnp.sum(weights, axis=1, keepdims=True)
    kept = jnp.where(picked, dots_all, 0.0)
    dense = gates * (kept - jnp.sum(gates * kept, axis=1, keepdims=True))
    cols = width // n
    mine = lax.dynamic_slice_in_dim(tok_all, me * cols, cols, axis=1)
    high = dense.astype(jnp.bfloat16)
    low = (dense - high.astype(jnp.float32)).astype(jnp.bfloat16)
    both = jnp.concatenate([high, low], axis=1)
    part = lax.dot_general(
        mine, both, (((0,), (0,)), ((), ())), preferred_element_type=jnp.float32
    )
    router_grad = lax.psum(part[:, :experts] + part[:, experts:], "dp")
    own = lax.dynamic_slice_in_dim(dots_all, me * tok_rows, tok_rows, axis=0)
    hits = (expert_index[:, :, None] == labels).astype(jnp.float32)
    gate_grad = jnp.sum(hits * own[:, None, :], axis=2)
    return (gate_grad, router_grad)


def solution(mesh):
    in_specs = (
        P(("dp", "expert"), None),
        P(("dp", "expert"), None),
        P(),
        P(("dp", "expert"), None),
        P("expert", None, None),
        P("expert", None, None),
        P("expert", None, None),
    )
    out_specs = (P(("dp", "expert"), None), P("expert", None))
    return jax.shard_map(
        on_device, mesh=mesh, in_specs=in_specs, out_specs=out_specs, check_vma=False
    )
```

```python
import functools

import jax
import jax.numpy as jnp
from jax import lax
from jax.experimental import pallas as pl
from jax.experimental.pallas import tpu as pltpu
from jax.sharding import PartitionSpec as P


def plain(tokens, grad_out, router_weight, expert_index, w_gate, w_up, w_down):
    tok_rows, width = tokens.shape
    top = expert_index.shape[1]
    experts = router_weight.shape[1]
    me = lax.axis_index("expert")
    n = lax.axis_size("expert")
    index_all = lax.all_gather(expert_index, "expert", axis=0, tiled=True)
    tok_all = lax.all_gather(tokens, "expert", axis=0, tiled=True)
    grad_all = lax.all_gather(grad_out, "expert", axis=0, tiled=True)
    gate_in = jnp.dot(tok_all, w_gate[0], preferred_element_type=jnp.float32)
    up_in = jnp.dot(tok_all, w_up[0], preferred_element_type=jnp.float32)
    hidden = jax.nn.silu(gate_in) * up_in
    back = lax.dot_general(
        grad_all, w_down[0], (((1,), (1,)), ((), ())), preferred_element_type=jnp.float32
    )
    dots = jnp.sum(hidden * back, axis=1)
    dots_all = lax.all_gather(dots, "expert", axis=0).T
    labels = jnp.arange(experts, dtype=jnp.int32)
    picked = jnp.any(index_all[:, :, None] == labels, axis=1)
    logits = jnp.dot(tok_all, router_weight, preferred_element_type=jnp.float32)
    weights = jnp.where(picked, jnp.exp(jnp.where(picked, logits, 0.0)), 0.0)
    gates = weights / jnp.sum(weights, axis=1, keepdims=True)
    kept = jnp.where(picked, dots_all, 0.0)
    dense = gates * (kept - jnp.sum(gates * kept, axis=1, keepdims=True))
    cols = width // n
    mine = lax.dynamic_slice_in_dim(tok_all, me * cols, cols, axis=1)
    high = dense.astype(jnp.bfloat16)
    low = (dense - high.astype(jnp.float32)).astype(jnp.bfloat16)
    both = jnp.concatenate([high, low], axis=1)
    part = lax.dot_general(
        mine, both, (((0,), (0,)), ((), ())), preferred_element_type=jnp.float32
    )
    router_grad = lax.psum(part[:, :experts] + part[:, experts:], "dp")
    own = lax.dynamic_slice_in_dim(dots_all, me * tok_rows, tok_rows, axis=0)
    hits = (expert_index[:, :, None] == labels).astype(jnp.float32)
    gate_grad = jnp.sum(hits * own[:, None, :], axis=2)
    return (gate_grad, router_grad)


def layer_kernel(n, dp, tok_in, grad_in, rw_in, idx_in, wg_in, wu_in, wd_in, gg_out, rg_out,
                 tok, grad, idx, wg, wu, wd, hid, eo, lg, dots, part,
                 s_t, r_t, s_a, r_a, s_c, r_c, s_i, r_i, s_d, r_d, s_w, r_w, s_p, r_p, loc):
    plane = n // 2
    line = plane // 2
    me = lax.axis_index("expert")
    xd = lax.axis_index("dp")
    c = me % 2
    q = me // 2
    y = q % 2
    z = q // 2
    rows, width = tok_in.shape
    ff = wg_in.shape[2]
    experts, top = rw_in.shape[0], idx_in.shape[0]
    cut = rows * 5 // 8
    pair = 2 * rows

    def dev(zz, yy, cc):
        return {"expert": (zz * 2 + yy) * 2 + cc}

    def remote(src, dst, ss, rs, where):
        return pltpu.make_async_remote_copy(
            src_ref=src, dst_ref=dst, send_sem=ss, recv_sem=rs,
            device_id=where, device_id_type=pl.DeviceIdType.MESH)

    DOWN, UP, SIDE = 0, 1, 2

    def target(way):
        if way == DOWN:
            return dev(z - 1, y, c)
        if way == UP:
            return dev(z + 1, y, c)
        return dev(z, 1 - y, c)

    kinds = {"t": (tok, tok_in, 0, rows, s_t, r_t),
             "a": (grad, grad_in, 0, cut, s_a, r_a),
             "c": (grad, grad_in, cut, rows - cut, s_c, r_c)}

    def piece(kind, zb, yb, way, own=False):
        buf, inp, lo, size, ss, rs = kinds[kind]
        at = buf.at[zb, pl.ds(pl.multiple_of(yb * rows + lo, 16), size)]
        src = inp.at[pl.ds(lo, size)] if own else at
        return remote(src, at, ss.at[zb * 2 + yb, way], rs.at[zb * 2 + yb], target(way))

    def arrived(kind, zb, yb):
        piece(kind, zb, yb, SIDE).wait_recv()

    barrier = pltpu.get_barrier_semaphore()

    def plane_dev(k):
        return {"expert": ((q + k) % plane) * 2 + c}

    def owner_dev(k):
        return {"dp": (xd + k // 2) % dp, "expert": q * 2 + (c + k) % 2}

    for k in range(1, plane):
        pl.semaphore_signal(barrier, inc=1, device_id=plane_dev(k), device_id_type=pl.DeviceIdType.MESH)
    for k in range(1, 2 * dp):
        pl.semaphore_signal(barrier, inc=1, device_id=owner_dev(k), device_id_type=pl.DeviceIdType.MESH)
    mine = pl.ds(pl.multiple_of(y * rows, 16), rows)
    local = [pltpu.make_async_copy(tok_in, tok.at[z, mine], loc.at[0]),
             pltpu.make_async_copy(grad_in, grad.at[z, mine], loc.at[1]),
             pltpu.make_async_copy(idx_in, idx.at[q], loc.at[2]),
             pltpu.make_async_copy(wg_in.at[0], wg.at[c], loc.at[3]),
             pltpu.make_async_copy(wu_in.at[0], wu.at[c], loc.at[4]),
             pltpu.make_async_copy(wd_in.at[0], wd.at[c], loc.at[5])]
    for copy in local:
        copy.start()
    pl.semaphore_wait(barrier, plane - 1 + 2 * dp - 1)

    def own_z(kind, way):
        piece(kind, z, y, way, own=True).start()

    pl.when(z > 0)(lambda: own_z("t", DOWN))
    pl.when(z < line - 1)(lambda: own_z("t", UP))
    own_z("t", SIDE)
    other = {"expert": q * 2 + (1 - c)}
    weights = [remote(wg_in.at[0], wg.at[c], s_w.at[0], r_w.at[0], other),
               remote(wu_in.at[0], wu.at[c], s_w.at[1], r_w.at[1], other),
               remote(wd_in.at[0], wd.at[c], s_w.at[2], r_w.at[2], other)]
    for w in weights:
        w.start()
    index_sends = [remote(idx_in, idx.at[q], s_i.at[k], r_i.at[k], plane_dev(k)) for k in range(1, plane)]
    for w in index_sends:
        w.start()
    pl.when(z == 0)(lambda: own_z("a", UP))
    pl.when(z == line - 1)(lambda: own_z("a", DOWN))

    def relay(kind, s):
        @pl.when(z + s < line)
        def _():
            arrived(kind, z + s, y)

            @pl.when(z > 0)
            def _():
                piece(kind, z + s, y, DOWN).start()
            piece(kind, z + s, y, SIDE).start()

        @pl.when(z - s >= 0)
        def _():
            arrived(kind, z - s, y)

            @pl.when(z < line - 1)
            def _():
                piece(kind, z - s, y, UP).start()
            piece(kind, z - s, y, SIDE).start()

    ft = ff // 3 if ff % 384 == 0 else ff
    dt = width // 4 if width % 512 == 0 else width

    def produce(zp):
        @pl.loop(0, 2)
        def _(r):
            @pl.loop(0, ff // ft)
            def _(j):
                at = pl.ds(pl.multiple_of(j * ft, 128), ft)
                x = tok[zp]
                g = jnp.dot(x, wg[r, :, at], preferred_element_type=jnp.float32)
                u = jnp.dot(x, wu[r, :, at], preferred_element_type=jnp.float32)
                hid[:, at] = (g / (1.0 + jnp.exp(-g)) * u).astype(jnp.bfloat16)

            @pl.loop(0, width // dt)
            def _(j):
                at = pl.ds(pl.multiple_of(j * dt, 128), dt)
                eo[zp, r, :, at] = jnp.dot(
                    hid[...], wd[r, :, at], preferred_element_type=jnp.float32).astype(jnp.bfloat16)
        lg[:, pl.ds(pl.multiple_of(zp * pair, 128), pair)] = lax.dot_general(
            rw_in[...], tok[zp], (((1,), (1,)), ((), ())), preferred_element_type=jnp.float32)

    def produce_ring(s):
        if s == 0:
            arrived("t", z, 1 - y)
            produce(z)
            return

        @pl.when(z + s < line)
        def _():
            arrived("t", z + s, 1 - y)
            produce(z + s)

        @pl.when(z - s >= 0)
        def _():
            arrived("t", z - s, 1 - y)
            produce(z - s)

    for s in range(1, line):
        relay("t", s)
        pl.when(z == s)(lambda: own_z("a", UP)) if s < line - 1 else None
        pl.when(line - 1 - z == s)(lambda: own_z("a", DOWN)) if s < line - 1 else None
        if s == line - 1:
            own_z("c", SIDE)
            own_z("a", SIDE)
        if s == 1:
            for copy in local:
                copy.wait()
            for w in weights:
                w.wait_recv()
        produce_ring(s - 1)

    for s in range(1, line):
        relay("a", s)
        if s == 1:
            produce_ring(line - 1)

    arrived("c", z, 1 - y)
    for yb in range(2):
        pl.when(z > 0)(lambda yb=yb: piece("c", z, yb, DOWN).start())
        pl.when(z < line - 1)(lambda yb=yb: piece("c", z, yb, UP).start())

    def reduce_pair(zp):
        @pl.loop(0, 2)
        def _(r):
            total = jnp.zeros((pair, 128), jnp.float32)
            for j in range(width // 128):
                at = pl.ds(j * 128, 128)
                total += eo[zp, r, :, at].astype(jnp.float32) * grad[zp, :, at].astype(jnp.float32)
            row = jnp.sum(total.T, axis=0, keepdims=True)
            dots[q, pl.ds(r, 1), pl.ds(pl.multiple_of(zp * pair, 128), pair)] = row

    arrived("a", z, 1 - y)
    reduce_pair(z)
    for s in range(1, line):
        def take(zb, way, ok):
            for yb in range(2):
                arrived("c", zb, yb)
                pl.when(ok)(lambda yb=yb: piece("c", zb, yb, way).start())

        pl.when(z + s < line)(lambda: take(z + s, DOWN, z > 0))
        pl.when(z - s >= 0)(lambda: take(z - s, UP, z < line - 1))

        @pl.when(z + s < line)
        def _():
            arrived("a", z + s, 1 - y)
            reduce_pair(z + s)

        @pl.when(z - s >= 0)
        def _():
            arrived("a", z - s, 1 - y)
            reduce_pair(z - s)

    dot_sends = [remote(dots.at[q], dots.at[q], s_d.at[k], r_d.at[k], plane_dev(k)) for k in range(1, plane)]
    for w in dot_sends:
        w.start()
    for w in index_sends:
        w.wait()
    labels = lax.broadcasted_iota(jnp.int32, (experts, plane * rows), 0)
    chosen = jnp.zeros((experts, plane * rows), jnp.float32)
    for k in range(top):
        named = jnp.concatenate([idx[b, pl.ds(k, 1), :] for b in range(plane)], axis=1)
        chosen = jnp.where(labels == named, 1.0, chosen)
    weight = jnp.where(chosen > 0.0, jnp.exp(jnp.where(chosen > 0.0, lg[...], 0.0)), 0.0)
    gates = weight / jnp.sum(weight, axis=0, keepdims=True)
    for w in dot_sends:
        w.wait()
    all_dots = jnp.concatenate([dots[b] for b in range(plane)], axis=0)
    kept = jnp.where(chosen > 0.0, all_dots, 0.0)
    dense = gates * (kept - jnp.sum(gates * kept, axis=0, keepdims=True))
    high = dense.astype(jnp.bfloat16)
    low = (dense - high.astype(jnp.float32)).astype(jnp.bfloat16)
    cols = width // n
    at = pl.ds(pl.multiple_of(q * 2 * cols, 128), 2 * cols)
    both = jnp.concatenate([high, low], axis=0)
    split = jnp.zeros((2 * experts, 2 * cols), jnp.float32)
    for b in range(line):
        split += jnp.dot(both[:, b * pair:(b + 1) * pair], tok[b, :, at], preferred_element_type=jnp.float32)
    terms = split[:experts] + split[experts:]
    part[0, 0] = terms[:, :cols]
    part[0, 1] = terms[:, cols:]
    part_sends = [remote(part.at[0, (c + k) % 2], part.at[k, 0], s_p.at[k], r_p.at[k], owner_dev(k))
                  for k in range(1, 2 * dp)]
    for w in part_sends:
        w.start()
    own = jnp.concatenate(
        [dots[b, :, pl.ds(pl.multiple_of(q * rows, 128), rows)] for b in range(plane)], axis=0)
    names = idx[q]
    small = lax.broadcasted_iota(jnp.int32, (experts, rows), 0)
    for k in range(top):
        gg_out[pl.ds(k, 1), :] = jnp.sum(
            jnp.where(small == names[k:k + 1, :], own, 0.0), axis=0, keepdims=True)
    for w in part_sends:
        w.wait()
    total = part[0, c]
    for k in range(1, 2 * dp):
        total += part[k, 0]
    rg_out[...] = total

    for w in weights:
        w.wait_send()

    def gone(kind, zb, yb, way):
        piece(kind, zb, yb, way).wait_send()

    for kind in ("t", "a"):
        for zb in range(line):
            pl.when((zb >= z) & (z > 0))(lambda: gone(kind, zb, y, DOWN))
            pl.when((zb <= z) & (z < line - 1))(lambda: gone(kind, zb, y, UP))
            gone(kind, zb, y, SIDE)
    gone("c", z, y, SIDE)
    for zb in range(line):
        for yb in range(2):
            pl.when((zb >= z) & (z > 0))(lambda: gone("c", zb, yb, DOWN))
            pl.when((zb <= z) & (z < line - 1))(lambda: gone("c", zb, yb, UP))


def fused(n, dp, tokens, grad_out, router_weight, expert_index, w_gate, w_up, w_down):
    rows, width = tokens.shape
    ff = w_gate.shape[2]
    top = expert_index.shape[1]
    experts = router_weight.shape[1]
    plane, cols = n // 2, width // n
    line = plane // 2
    pair = 2 * rows
    anywhere = pl.BlockSpec(memory_space=pl.ANY)
    vmem = pl.BlockSpec(memory_space=pltpu.VMEM)
    dma = pltpu.SemaphoreType.DMA
    bf, f32 = jnp.bfloat16, jnp.float32
    gg, rg = pl.pallas_call(
        functools.partial(layer_kernel, n, dp),
        out_shape=(jax.ShapeDtypeStruct((top, rows), f32), jax.ShapeDtypeStruct((experts, cols), f32)),
        in_specs=[anywhere, anywhere, vmem, vmem, anywhere, anywhere, anywhere],
        out_specs=(vmem, vmem),
        scratch_shapes=[
            pltpu.VMEM((line, pair, width), bf),
            pltpu.VMEM((line, pair, width), bf),
            pltpu.VMEM((plane, top, rows), jnp.int32),
            pltpu.VMEM((2, width, ff), bf),
            pltpu.VMEM((2, width, ff), bf),
            pltpu.VMEM((2, ff, width), bf),
            pltpu.VMEM((pair, ff), bf),
            pltpu.VMEM((line, 2, pair, width), bf),
            pltpu.VMEM((experts, plane * rows), f32),
            pltpu.VMEM((plane, 2, plane * rows), f32),
            pltpu.VMEM((2 * dp, 2, experts, cols), f32),
            dma((plane, 3)), dma((plane,)), dma((plane, 3)), dma((plane,)), dma((plane, 3)), dma((plane,)),
            dma((plane,)), dma((plane,)), dma((plane,)), dma((plane,)),
            dma((3,)), dma((3,)), dma((2 * dp,)), dma((2 * dp,)), dma((6,)),
        ],
        compiler_params=pltpu.CompilerParams(
            collective_id=0, has_side_effects=True, vmem_limit_bytes=60 * 2**20),
    )(tokens, grad_out, router_weight.T, expert_index.T, w_gate, w_up, w_down)
    return gg.T, rg.T


def solution(mesh):
    n, dp = mesh.shape["expert"], mesh.shape["dp"]

    def on_device(tokens, grad_out, router_weight, expert_index, w_gate, w_up, w_down):
        rows, width = tokens.shape
        ff = w_gate.shape[2]
        held = 2 * (2 * n // 2 * rows * width * 2 + 6 * ff * width)
        fits = n % 4 == 0 and n >= 8 and held < 44 * 2**20 and width % (128 * n) == 0
        fits = fits and rows % 128 == 0 and router_weight.shape[1] == n
        body = functools.partial(fused, n, dp) if fits else plain
        return body(tokens, grad_out, router_weight, expert_index, w_gate, w_up, w_down)

    in_specs = (
        P(("dp", "expert"), None),
        P(("dp", "expert"), None),
        P(),
        P(("dp", "expert"), None),
        P("expert", None, None),
        P("expert", None, None),
        P("expert", None, None),
    )
    out_specs = (P(("dp", "expert"), None), P("expert", None))
    return jax.shard_map(
        on_device, mesh=mesh, in_specs=in_specs, out_specs=out_specs, check_vma=False
    )
```

```python
import functools

import jax
import jax.numpy as jnp
from jax import lax
from jax.experimental import pallas as pl
from jax.experimental.pallas import tpu as pltpu
from jax.sharding import PartitionSpec as P


def plain(tokens, grad_out, router_weight, expert_index, w_gate, w_up, w_down):
    tok_rows, width = tokens.shape
    top = expert_index.shape[1]
    experts = router_weight.shape[1]
    me = lax.axis_index("expert")
    n = lax.axis_size("expert")
    index_all = lax.all_gather(expert_index, "expert", axis=0, tiled=True)
    tok_all = lax.all_gather(tokens, "expert", axis=0, tiled=True)
    grad_all = lax.all_gather(grad_out, "expert", axis=0, tiled=True)
    gate_in = jnp.dot(tok_all, w_gate[0], preferred_element_type=jnp.float32)
    up_in = jnp.dot(tok_all, w_up[0], preferred_element_type=jnp.float32)
    hidden = jax.nn.silu(gate_in) * up_in
    back = lax.dot_general(
        grad_all, w_down[0], (((1,), (1,)), ((), ())), preferred_element_type=jnp.float32
    )
    dots = jnp.sum(hidden * back, axis=1)
    dots_all = lax.all_gather(dots, "expert", axis=0).T
    labels = jnp.arange(experts, dtype=jnp.int32)
    picked = jnp.any(index_all[:, :, None] == labels, axis=1)
    logits = jnp.dot(tok_all, router_weight, preferred_element_type=jnp.float32)
    weights = jnp.where(picked, jnp.exp(jnp.where(picked, logits, 0.0)), 0.0)
    gates = weights / jnp.sum(weights, axis=1, keepdims=True)
    kept = jnp.where(picked, dots_all, 0.0)
    dense = gates * (kept - jnp.sum(gates * kept, axis=1, keepdims=True))
    cols = width // n
    mine = lax.dynamic_slice_in_dim(tok_all, me * cols, cols, axis=1)
    high = dense.astype(jnp.bfloat16)
    low = (dense - high.astype(jnp.float32)).astype(jnp.bfloat16)
    both = jnp.concatenate([high, low], axis=1)
    part = lax.dot_general(
        mine, both, (((0,), (0,)), ((), ())), preferred_element_type=jnp.float32
    )
    router_grad = lax.psum(part[:, :experts] + part[:, experts:], "dp")
    own = lax.dynamic_slice_in_dim(dots_all, me * tok_rows, tok_rows, axis=0)
    hits = (expert_index[:, :, None] == labels).astype(jnp.float32)
    gate_grad = jnp.sum(hits * own[:, None, :], axis=2)
    return (gate_grad, router_grad)


def layer_kernel(n, dp, tok_in, grad_in, rw_in, idx_in, wg_in, wu_in, wd_in, gg_out, rg_out,
                 tok, grad, idx, wg, wu, wd, hid, eo, lg, dots, part,
                 s_t, r_t, s_a, r_a, s_c, r_c, s_i, r_i, s_d, r_d, s_w, r_w, s_p, r_p, loc):
    plane = n // 2
    line = plane // 2
    me = lax.axis_index("expert")
    xd = lax.axis_index("dp")
    c = me % 2
    q = me // 2
    y = q % 2
    z = q // 2
    rows, width = tok_in.shape
    ff = wg_in.shape[2]
    experts, top = rw_in.shape[0], idx_in.shape[0]
    cut = rows * 5 // 8
    pair = 2 * rows

    def dev(zz, yy, cc):
        return {"expert": (zz * 2 + yy) * 2 + cc}

    def remote(src, dst, ss, rs, where):
        return pltpu.make_async_remote_copy(
            src_ref=src, dst_ref=dst, send_sem=ss, recv_sem=rs,
            device_id=where, device_id_type=pl.DeviceIdType.MESH)

    DOWN, UP, SIDE = 0, 1, 2

    def target(way):
        if way == DOWN:
            return dev(z - 1, y, c)
        if way == UP:
            return dev(z + 1, y, c)
        return dev(z, 1 - y, c)

    kinds = {"t": (tok, tok_in, 0, rows, s_t, r_t),
             "a": (grad, grad_in, 0, cut, s_a, r_a),
             "c": (grad, grad_in, cut, rows - cut, s_c, r_c)}

    def piece(kind, zb, yb, way, own=False):
        buf, inp, lo, size, ss, rs = kinds[kind]
        at = buf.at[zb, pl.ds(pl.multiple_of(yb * rows + lo, 16), size)]
        src = inp.at[pl.ds(lo, size)] if own else at
        return remote(src, at, ss.at[zb * 2 + yb, way], rs.at[zb * 2 + yb], target(way))

    def arrived(kind, zb, yb):
        piece(kind, zb, yb, SIDE).wait_recv()

    barrier = pltpu.get_barrier_semaphore()

    def plane_dev(k):
        return {"expert": ((q + k) % plane) * 2 + c}

    def owner_dev(k):
        return {"dp": (xd + k // 2) % dp, "expert": q * 2 + (c + k) % 2}

    for k in range(1, plane):
        pl.semaphore_signal(barrier, inc=1, device_id=plane_dev(k), device_id_type=pl.DeviceIdType.MESH)
    for k in range(1, 2 * dp):
        pl.semaphore_signal(barrier, inc=1, device_id=owner_dev(k), device_id_type=pl.DeviceIdType.MESH)
    mine = pl.ds(pl.multiple_of(y * rows, 16), rows)
    local = [pltpu.make_async_copy(tok_in, tok.at[z, mine], loc.at[0]),
             pltpu.make_async_copy(grad_in, grad.at[z, mine], loc.at[1]),
             pltpu.make_async_copy(idx_in, idx.at[q], loc.at[2]),
             pltpu.make_async_copy(wg_in.at[0], wg.at[c], loc.at[3]),
             pltpu.make_async_copy(wu_in.at[0], wu.at[c], loc.at[4]),
             pltpu.make_async_copy(wd_in.at[0], wd.at[c], loc.at[5])]
    for copy in local:
        copy.start()
    pl.semaphore_wait(barrier, plane - 1 + 2 * dp - 1)

    def own_z(kind, way):
        piece(kind, z, y, way, own=True).start()

    pl.when(z > 0)(lambda: own_z("t", DOWN))
    pl.when(z < line - 1)(lambda: own_z("t", UP))
    own_z("t", SIDE)
    other = {"expert": q * 2 + (1 - c)}
    weights = [remote(wg_in.at[0], wg.at[c], s_w.at[0], r_w.at[0], other),
               remote(wu_in.at[0], wu.at[c], s_w.at[1], r_w.at[1], other),
               remote(wd_in.at[0], wd.at[c], s_w.at[2], r_w.at[2], other)]
    for w in weights:
        w.start()
    index_sends = [remote(idx_in, idx.at[q], s_i.at[k], r_i.at[k], plane_dev(k)) for k in range(1, plane)]
    for w in index_sends:
        w.start()
    pl.when(z > 0)(lambda: own_z("a", DOWN))
    pl.when(z < line - 1)(lambda: own_z("a", UP))
    own_z("c", SIDE)

    def relay(kind, s):
        @pl.when(z + s < line)
        def _():
            arrived(kind, z + s, y)

            @pl.when(z > 0)
            def _():
                piece(kind, z + s, y, DOWN).start()
            piece(kind, z + s, y, SIDE).start()

        @pl.when(z - s >= 0)
        def _():
            arrived(kind, z - s, y)

            @pl.when(z < line - 1)
            def _():
                piece(kind, z - s, y, UP).start()
            piece(kind, z - s, y, SIDE).start()

    ft = ff // 3 if ff % 384 == 0 else ff
    dt = width // 4 if width % 512 == 0 else width

    def produce(zp):
        @pl.loop(0, 2)
        def _(r):
            @pl.loop(0, ff // ft)
            def _(j):
                at = pl.ds(pl.multiple_of(j * ft, 128), ft)
                x = tok[zp]
                g = jnp.dot(x, wg[r, :, at], preferred_element_type=jnp.float32)
                u = jnp.dot(x, wu[r, :, at], preferred_element_type=jnp.float32)
                hid[:, at] = (g / (1.0 + jnp.exp(-g)) * u).astype(jnp.bfloat16)

            @pl.loop(0, width // dt)
            def _(j):
                at = pl.ds(pl.multiple_of(j * dt, 128), dt)
                eo[zp, r, :, at] = jnp.dot(
                    hid[...], wd[r, :, at], preferred_element_type=jnp.float32).astype(jnp.bfloat16)
        lg[:, pl.ds(pl.multiple_of(zp * pair, 128), pair)] = lax.dot_general(
            rw_in[...], tok[zp], (((1,), (1,)), ((), ())), preferred_element_type=jnp.float32)

    def produce_ring(s):
        if s == 0:
            arrived("t", z, 1 - y)
            produce(z)
            return

        @pl.when(z + s < line)
        def _():
            arrived("t", z + s, 1 - y)
            produce(z + s)

        @pl.when(z - s >= 0)
        def _():
            arrived("t", z - s, 1 - y)
            produce(z - s)

    relay("t", 1)
    for copy in local:
        copy.wait()
    for w in weights:
        w.wait_recv()
    produce_ring(0)
    for s in range(2, line):
        relay("t", s)
    own_z("a", SIDE)
    arrived("c", z, 1 - y)
    for yb in range(2):
        pl.when(z > 0)(lambda yb=yb: piece("c", z, yb, DOWN).start())
        pl.when(z < line - 1)(lambda yb=yb: piece("c", z, yb, UP).start())

    for s in range(1, line):
        relay("a", s)
        produce_ring(s)

    def reduce_pair(zp):
        @pl.loop(0, 2)
        def _(r):
            total = jnp.zeros((pair, 128), jnp.float32)
            for j in range(width // 128):
                at = pl.ds(j * 128, 128)
                total += eo[zp, r, :, at].astype(jnp.float32) * grad[zp, :, at].astype(jnp.float32)
            row = jnp.sum(total.T, axis=0, keepdims=True)
            dots[q, pl.ds(r, 1), pl.ds(pl.multiple_of(zp * pair, 128), pair)] = row

    arrived("a", z, 1 - y)
    reduce_pair(z)
    for s in range(1, line):
        def take(zb, way, ok):
            for yb in range(2):
                arrived("c", zb, yb)
                pl.when(ok)(lambda yb=yb: piece("c", zb, yb, way).start())

        pl.when(z + s < line)(lambda: take(z + s, DOWN, z > 0))
        pl.when(z - s >= 0)(lambda: take(z - s, UP, z < line - 1))

        @pl.when(z + s < line)
        def _():
            arrived("a", z + s, 1 - y)
            reduce_pair(z + s)

        @pl.when(z - s >= 0)
        def _():
            arrived("a", z - s, 1 - y)
            reduce_pair(z - s)

    dot_sends = [remote(dots.at[q], dots.at[q], s_d.at[k], r_d.at[k], plane_dev(k)) for k in range(1, plane)]
    for w in dot_sends:
        w.start()
    for w in index_sends:
        w.wait()
    labels = lax.broadcasted_iota(jnp.int32, (experts, plane * rows), 0)
    chosen = jnp.zeros((experts, plane * rows), jnp.float32)
    for k in range(top):
        named = jnp.concatenate([idx[b, pl.ds(k, 1), :] for b in range(plane)], axis=1)
        chosen = jnp.where(labels == named, 1.0, chosen)
    weight = jnp.where(chosen > 0.0, jnp.exp(jnp.where(chosen > 0.0, lg[...], 0.0)), 0.0)
    gates = weight / jnp.sum(weight, axis=0, keepdims=True)
    for w in dot_sends:
        w.wait()
    all_dots = jnp.concatenate([dots[b] for b in range(plane)], axis=0)
    kept = jnp.where(chosen > 0.0, all_dots, 0.0)
    dense = gates * (kept - jnp.sum(gates * kept, axis=0, keepdims=True))
    high = dense.astype(jnp.bfloat16)
    low = (dense - high.astype(jnp.float32)).astype(jnp.bfloat16)
    cols = width // n
    at = pl.ds(pl.multiple_of(q * 2 * cols, 128), 2 * cols)
    both = jnp.concatenate([high, low], axis=0)
    split = jnp.zeros((2 * experts, 2 * cols), jnp.float32)
    for b in range(line):
        split += jnp.dot(both[:, b * pair:(b + 1) * pair], tok[b, :, at], preferred_element_type=jnp.float32)
    terms = split[:experts] + split[experts:]
    part[0, 0] = terms[:, :cols]
    part[0, 1] = terms[:, cols:]
    part_sends = [remote(part.at[0, (c + k) % 2], part.at[k, 0], s_p.at[k], r_p.at[k], owner_dev(k))
                  for k in range(1, 2 * dp)]
    for w in part_sends:
        w.start()
    own = jnp.concatenate(
        [dots[b, :, pl.ds(pl.multiple_of(q * rows, 128), rows)] for b in range(plane)], axis=0)
    names = idx[q]
    small = lax.broadcasted_iota(jnp.int32, (experts, rows), 0)
    for k in range(top):
        gg_out[pl.ds(k, 1), :] = jnp.sum(
            jnp.where(small == names[k:k + 1, :], own, 0.0), axis=0, keepdims=True)
    for w in part_sends:
        w.wait()
    total = part[0, c]
    for k in range(1, 2 * dp):
        total += part[k, 0]
    rg_out[...] = total

    for w in weights:
        w.wait_send()

    def gone(kind, zb, yb, way):
        piece(kind, zb, yb, way).wait_send()

    for kind in ("t", "a"):
        for zb in range(line):
            pl.when((zb >= z) & (z > 0))(lambda: gone(kind, zb, y, DOWN))
            pl.when((zb <= z) & (z < line - 1))(lambda: gone(kind, zb, y, UP))
            gone(kind, zb, y, SIDE)
    gone("c", z, y, SIDE)
    for zb in range(line):
        for yb in range(2):
            pl.when((zb >= z) & (z > 0))(lambda: gone("c", zb, yb, DOWN))
            pl.when((zb <= z) & (z < line - 1))(lambda: gone("c", zb, yb, UP))


def fused(n, dp, tokens, grad_out, router_weight, expert_index, w_gate, w_up, w_down):
    rows, width = tokens.shape
    ff = w_gate.shape[2]
    top = expert_index.shape[1]
    experts = router_weight.shape[1]
    plane, cols = n // 2, width // n
    line = plane // 2
    pair = 2 * rows
    anywhere = pl.BlockSpec(memory_space=pl.ANY)
    vmem = pl.BlockSpec(memory_space=pltpu.VMEM)
    dma = pltpu.SemaphoreType.DMA
    bf, f32 = jnp.bfloat16, jnp.float32
    gg, rg = pl.pallas_call(
        functools.partial(layer_kernel, n, dp),
        out_shape=(jax.ShapeDtypeStruct((top, rows), f32), jax.ShapeDtypeStruct((experts, cols), f32)),
        in_specs=[anywhere, anywhere, vmem, vmem, anywhere, anywhere, anywhere],
        out_specs=(vmem, vmem),
        scratch_shapes=[
            pltpu.VMEM((line, pair, width), bf),
            pltpu.VMEM((line, pair, width), bf),
            pltpu.VMEM((plane, top, rows), jnp.int32),
            pltpu.VMEM((2, width, ff), bf),
            pltpu.VMEM((2, width, ff), bf),
            pltpu.VMEM((2, ff, width), bf),
            pltpu.VMEM((pair, ff), bf),
            pltpu.VMEM((line, 2, pair, width), bf),
            pltpu.VMEM((experts, plane * rows), f32),
            pltpu.VMEM((plane, 2, plane * rows), f32),
            pltpu.VMEM((2 * dp, 2, experts, cols), f32),
            dma((plane, 3)), dma((plane,)), dma((plane, 3)), dma((plane,)), dma((plane, 3)), dma((plane,)),
            dma((plane,)), dma((plane,)), dma((plane,)), dma((plane,)),
            dma((3,)), dma((3,)), dma((2 * dp,)), dma((2 * dp,)), dma((6,)),
        ],
        compiler_params=pltpu.CompilerParams(
            collective_id=0, has_side_effects=True, vmem_limit_bytes=60 * 2**20),
    )(tokens, grad_out, router_weight.T, expert_index.T, w_gate, w_up, w_down)
    return gg.T, rg.T


def solution(mesh):
    n, dp = mesh.shape["expert"], mesh.shape["dp"]

    def on_device(tokens, grad_out, router_weight, expert_index, w_gate, w_up, w_down):
        rows, width = tokens.shape
        ff = w_gate.shape[2]
        held = 2 * (2 * n // 2 * rows * width * 2 + 6 * ff * width)
        fits = n % 4 == 0 and n >= 8 and held < 44 * 2**20 and width % (128 * n) == 0
        fits = fits and rows % 128 == 0 and router_weight.shape[1] == n
        body = functools.partial(fused, n, dp) if fits else plain
        return body(tokens, grad_out, router_weight, expert_index, w_gate, w_up, w_down)

    in_specs = (
        P(("dp", "expert"), None),
        P(("dp", "expert"), None),
        P(),
        P(("dp", "expert"), None),
        P("expert", None, None),
        P("expert", None, None),
        P("expert", None, None),
    )
    out_specs = (P(("dp", "expert"), None), P("expert", None))
    return jax.shard_map(
        on_device, mesh=mesh, in_specs=in_specs, out_specs=out_specs, check_vma=False
    )
```
